256 devices in a mesh: groups: 2 (over y), freq: 128 (over z, x, core).
Axes of the slice: x: 4, y: 2, z: 16, core: 2. Of those that a mesh axis runs over, the one named last changes fastest.
The devices are a block of a 4x16x16 slice.
Arguments:
- primary_one: bfloat16 [1024, 512, 512], P(('groups', 'freq')), parts along dimension 0, may hold values from -6 to 6
- primary_two: bfloat16 [1024, 512, 512], P(('groups', 'freq')), parts along dimension 0, may hold values from -6 to 6
- primary_three: bfloat16 [1024, 512, 512], P(('groups', 'freq')), parts along dimension 0, may hold values from -6 to 6
- window_start: int32 [3, 1024, 512], P(None, ('groups', 'freq')), parts along dimension 1, may hold values from 0 to 255
- window_end: int32 [3, 1024, 512], P(None, ('groups', 'freq')), parts along dimension 1, may hold values from 257 to 512
Outputs:
- predicted: bfloat16 [1024, 512, 512], P(('groups', 'freq')), parts along dimension 0
The draws below stay inside these ranges and needn't reach their ends.
There are 2 independent parts, one for each index of `groups`. The reference program is written for one: setup_inputs(seed, part) draws one part's arguments, and reference() takes and returns one part's arrays. A program takes and returns all parts, laid end to end along the dimension named above; each array names one. Nothing has to cross between parts.
Inputs may be any that keep to these rules, and one draw needn't show every extreme that they name: window_start of a trace is below its window_end.
All inputs are finite; a program needn't handle non-finite values.
Results may differ from the reference program's by a relative error of at most 0.0089.
Values may be sent and summed in bfloat16 or wider, within the bound.
A program may use at most 64 MiB of HBM per device.

```python
import jax
import jax.numpy as jnp
from jax import lax

NS = 512
NR = 512
NT = 512
NF = 128


def touch_ends(result, stream_key, least, high):
    index_at = [jax.random.randint(jax.random.fold_in(stream_key, axis), (), 0, length) for axis, length in enumerate(result.shape)]
    widest = result.shape.index(max(result.shape))
    beside = index_at[:widest] + [(index_at[widest] + 1) % result.shape[widest]] + index_at[widest + 1:]
    return result.at[tuple(index_at)].set(least).at[tuple(beside)].set(high)


def steps_of(stream_key, shape, cuts, low, largest):
    level = 1.0
    for dim, parts in cuts:
        steps = jax.random.uniform(jax.random.fold_in(jax.random.fold_in(stream_key, 6), dim), (parts,), jnp.float32, low / len(cuts), largest / len(cuts))
        level = level * jnp.repeat(jnp.exp(steps), shape[dim] // parts).reshape((-1,) + (1,) * (len(shape) - 1 - dim))
    return level


def centred(stream_key, shape, spread, reach, pieces=(), kind=jnp.bfloat16):
    gain = steps_of(stream_key, shape, pieces, -0.22, 0.18) if pieces else 1.0
    entries = jax.random.normal(stream_key, shape, jnp.float32) * spread * gain
    return jnp.minimum(jnp.maximum(entries, -reach), reach).astype(kind)


def setup_inputs(seed: int = 0, part: int = 0) -> dict:
    streams_of = jax.random.split(jax.random.key(seed), 6)
    part_splits = jax.random.split(jax.random.fold_in(streams_of[5], part), 6)
    return {
        "primary_one": centred(part_splits[0], (NS, NR, NT), 1.0, 6.0, ((0, 128),)),
        "primary_two": centred(part_splits[1], (NS, NR, NT), 1.0, 6.0, ((0, 128),)),
        "primary_three": centred(part_splits[2], (NS, NR, NT), 1.0, 6.0, ((0, 128),)),
        "window_start": touch_ends(jax.random.randint(part_splits[3], (3, NS, NR), 0, NT // 2), jax.random.fold_in(part_splits[3], 1), 0, (NT // 2) - 1).astype(jnp.int32),
        "window_end": touch_ends(jax.random.randint(part_splits[4], (3, NS, NR), NT // 2 + 1, NT + 1), jax.random.fold_in(part_splits[4], 1), NT // 2 + 1, NT).astype(jnp.int32),
    }


def make_table(count, samples):
    waves = jnp.arange(1, count + 1, dtype=jnp.int32)[:, None]
    times = jnp.arange(samples, dtype=jnp.int32)[None, :]
    phase = waves * times % samples
    angle = 2.0 * jnp.pi / samples * phase.astype(jnp.float32)
    both = jnp.stack([jnp.cos(angle), -jnp.sin(angle)], axis=1)
    return both.reshape(2 * count, samples).astype(jnp.bfloat16)

def spectrum(traces, start, finish, table):
    times = jnp.arange(NT, dtype=jnp.int32)
    inside = (times >= start[:, :, None]) & (times < finish[:, :, None])
    windowed = jnp.where(inside, traces, jnp.zeros_like(traces))
    flat = windowed.reshape(NS * NR, NT)
    spec = lax.dot_general(table, flat, (((1,), (1,)), ((), ())), preferred_element_type=jnp.float32)
    spec = spec * (1.0 / jnp.sqrt(jnp.float32(NT)))
    return spec.astype(jnp.bfloat16).reshape(NF, 2, NS, NR)

def slice_product(items):
    first, second, third = items
    first = first.astype(jnp.float32)
    second = second.astype(jnp.float32)
    third = third.astype(jnp.float32)
    high = lax.Precision.HIGHEST
    cross_re = jnp.dot(first[0], second[0].T, precision=high) + jnp.dot(first[1], second[1].T, precision=high)
    cross_im = jnp.dot(first[1], second[0].T, precision=high) - jnp.dot(first[0], second[1].T, precision=high)
    cross = (jnp.stack([cross_re, cross_im]) * (1.0 / jnp.sqrt(jnp.float32(NR)))).astype(jnp.bfloat16)
    cross = cross.astype(jnp.float32)
    mult_re = jnp.dot(cross[0], third[0], precision=high) - jnp.dot(cross[1], third[1], precision=high)
    mult_im = jnp.dot(cross[0], third[1], precision=high) + jnp.dot(cross[1], third[0], precision=high)
    return (jnp.stack([mult_re, mult_im]) * (1.0 / jnp.sqrt(jnp.float32(NS)))).astype(jnp.bfloat16)

def reference(primary_one, primary_two, primary_three, window_start, window_end):
    table = make_table(NF, NT)
    spec_one = spectrum(primary_one, window_start[0], window_end[0], table)
    spec_two = spectrum(primary_two, window_start[1], window_end[1], table)
    spec_three = spectrum(primary_three, window_start[2], window_end[2], table)
    multiple = lax.map(slice_product, (spec_one, spec_two, spec_three))
    flat = multiple.reshape(2 * NF, NS * NR)
    timed = lax.dot_general(flat, table, (((0,), (0,)), ((), ())), preferred_element_type=jnp.float32)
    timed = timed * (1.0 / jnp.sqrt(jnp.float32(NF)))
    return timed.astype(jnp.bfloat16).reshape(NS, NR, NT)
```

```python
import functools

import jax
import jax.numpy as jnp
import numpy as np
from jax import lax
from jax.experimental import pallas as pl
from jax.experimental.pallas import tpu as pltpu
from jax.sharding import PartitionSpec as P

MESH = pl.DeviceIdType.MESH
LANES = 128
ROW = 8
F32 = jnp.float32
BF16 = jnp.bfloat16


def make_table(count, samples):
    waves = np.arange(1, count + 1, dtype=np.int64)[:, None]
    times = np.arange(samples, dtype=np.int64)[None, :]
    angle = np.float32(2.0 * np.pi / samples) * (waves * times % samples).astype(np.float32)
    both = np.concatenate([np.cos(angle), -np.sin(angle)], axis=0)
    return both.astype(BF16)


def shift_of(block):
    return ((block + 1) // 2) * (2 * (block % 2) - 1)


def kernel(
    size, p1, p2, p3, ws, we, tab_hbm, out_hbm,
    inp, wsv, wev, tab, a32, b32, s23, s1, r23, r1, xm, ym, zm, w, o, m, m32, outv,
    in_sem, out_sem, ssem23, ssem1, ssemo, rsem23, rsem1, rsemo,
):
    me = lax.axis_index("freq")
    group = lax.axis_index("groups")
    rows = size // ROW
    z, xc = me // ROW, me % ROW
    samples = tab.shape[1]
    sources, receivers = inp.shape[1], inp.shape[2]
    per = 2 * sources

    barrier = pltpu.get_barrier_semaphore()

    def greet(k, carry):
        pl.semaphore_signal(barrier, inc=1, device_id=(group, (me + k) % size), device_id_type=MESH)
        return carry

    loads = [
        pltpu.make_async_copy(ws, wsv, in_sem.at[0]),
        pltpu.make_async_copy(we, wev, in_sem.at[1]),
        pltpu.make_async_copy(tab_hbm, tab, in_sem.at[2]),
        pltpu.make_async_copy(p2, inp.at[1], in_sem.at[4]),
        pltpu.make_async_copy(p3, inp.at[2], in_sem.at[5]),
        pltpu.make_async_copy(p1, inp.at[0], in_sem.at[3]),
    ]
    for load in loads:
        load.start()
    lax.fori_loop(1, size, greet, 0)
    for load in loads[:3]:
        load.wait()

    def spectra(j, into, base, stride):
        ends = jnp.concatenate([wsv[j], wev[j]], axis=0).astype(F32)
        columns = ends.T
        times = lax.broadcasted_iota(jnp.int32, (receivers, samples), 1).astype(F32)
        for s in range(sources):
            first = columns[:, s : s + 1]
            last = columns[:, sources + s : sources + s + 1]
            inside = (times >= first) & (times < last)
            traces = jnp.where(inside, inp[j, s].astype(F32), 0.0).astype(BF16)
            spec = lax.dot_general(tab[...], traces, (((1,), (1,)), ((), ())), preferred_element_type=F32)
            spec = spec * np.float32(1.0 / np.sqrt(samples))
            for c in range(2):
                for q in range(receivers // LANES):
                    into[q, pl.ds(base + c * sources + s, size, stride=stride), :] = spec[
                        c * size : (c + 1) * size, q * LANES : (q + 1) * LANES
                    ]

    def each_partner(body):
        def step(i, carry):
            block, turn = i // ROW, i % ROW
            dst = ((z + shift_of(block) + rows) % rows) * ROW + (xc + turn) % ROW
            body(block, dst)
            return carry

        lax.fori_loop(1, size, step, 0)

    loads[3].wait()
    spectra(1, a32, 0, 2 * per)
    loads[4].wait()
    spectra(2, a32, per, 2 * per)

    def round23(i, carry):
        at = pl.multiple_of(i * ROW, ROW)
        lines = pl.ds(pl.multiple_of(i * ROW * 2 * per, ROW * 2 * per), ROW * 2 * per)
        for q in range(receivers // LANES):
            piece = a32[q, lines, :].reshape(ROW, 2 * per, LANES)
            s23[pl.ds(at, ROW), :, q * LANES : (q + 1) * LANES] = piece.astype(BF16)
        return carry

    lax.fori_loop(0, rows, round23, 0)
    pl.semaphore_wait(barrier, size - 1)

    def send23(block, dst):
        pltpu.make_async_remote_copy(
            s23.at[dst], r23.at[me], ssem23, rsem23, device_id=(group, dst), device_id_type=MESH
        ).start()

    each_partner(send23)
    r23[me] = s23[me]

    loads[5].wait()
    spectra(0, b32, 0, per)

    def round1(i, carry):
        at = pl.multiple_of(i * ROW, ROW)
        lines = pl.ds(pl.multiple_of(i * ROW * per, ROW * per), ROW * per)
        for q in range(receivers // LANES):
            piece = b32[q, lines, :].reshape(ROW, per, LANES)
            s1[pl.ds(at, ROW), :, q * LANES : (q + 1) * LANES] = piece.astype(BF16)
        return carry

    lax.fori_loop(0, rows, round1, 0)

    def send1(block, dst):
        pltpu.make_async_remote_copy(
            s1.at[dst], r1.at[me], ssem1, rsem1.at[block], device_id=(group, dst), device_id_type=MESH
        ).start()

    each_partner(send1)
    r1[me] = s1[me]

    pltpu.make_async_copy(s23.at[pl.ds(0, size - 1)], r23.at[pl.ds(0, size - 1)], rsem23).wait()
    half = lax.broadcasted_iota(jnp.int32, (ROW, per, receivers), 1)
    sign = jnp.where(half < sources, 1.0, -1.0).astype(F32)

    def arrange(i, carry):
        at = pl.multiple_of(i * ROW, ROW)
        to = pl.ds(pl.multiple_of(i * ROW * per, ROW * per), ROW * per)
        piece = r23[pl.ds(at, ROW)].astype(F32)
        second, third = piece[:, :per], piece[:, per:]
        turned = jnp.concatenate([third[:, sources:], third[:, :sources]], axis=1) * sign
        xm[to, :] = second.reshape(ROW * per, receivers).astype(BF16)
        ym[to, :] = third.reshape(ROW * per, receivers).astype(BF16)
        zm[to, :] = turned.reshape(ROW * per, receivers).astype(BF16)
        return carry

    lax.fori_loop(0, rows, arrange, 0)
    scale = np.float32(1.0 / np.sqrt(size * sources))

    def weigh(i, carry):
        at = pl.ds(pl.multiple_of(i * LANES, LANES), LANES)
        left = xm[:, at]
        dims = (((0,), (0,)), ((), ()))
        w[at, :receivers] = (lax.dot_general(left, ym[...], dims, preferred_element_type=F32) * scale).astype(BF16)
        w[at, receivers:] = (lax.dot_general(left, zm[...], dims, preferred_element_type=F32) * scale).astype(BF16)
        return carry

    lax.fori_loop(0, receivers // LANES, weigh, 0)
    scale1 = np.float32(1.0 / np.sqrt(receivers))

    def multiply(block, carry):
        came = ((z - shift_of(block) + rows) % rows) * ROW

        @pl.when(block == 0)
        def _():
            pltpu.make_async_copy(s1.at[pl.ds(0, ROW - 1)], r1.at[pl.ds(0, ROW - 1)], rsem1.at[block]).wait()

        @pl.when(block > 0)
        def _():
            pltpu.make_async_copy(s1.at[pl.ds(0, ROW)], r1.at[pl.ds(0, ROW)], rsem1.at[block]).wait()

        at = pl.ds(pl.multiple_of(came, ROW), ROW)
        piece = r1[at].astype(F32).reshape(ROW * per, receivers).astype(BF16)
        both = jnp.dot(piece, w[...], preferred_element_type=F32)
        a = both[:, :receivers].reshape(ROW, per, receivers)
        b = both[:, receivers:].reshape(ROW, per, receivers)
        turned = jnp.concatenate([b[:, sources:], b[:, :sources]], axis=1) * sign
        o[at] = ((a - turned) * scale1).astype(BF16)

        def back(turn, c):
            dst = came + (xc + turn) % ROW

            @pl.when(dst != me)
            def _():
                pltpu.make_async_remote_copy(
                    o.at[dst], m.at[me], ssemo, rsemo.at[block], device_id=(group, dst), device_id_type=MESH
                ).start()

            return c

        lax.fori_loop(0, ROW, back, 0)
        return carry

    lax.fori_loop(0, rows, multiply, 0)
    m[me] = o[me]

    def collect(block, carry):
        came = ((z + shift_of(block) + rows) % rows) * ROW

        @pl.when(block == 0)
        def _():
            pltpu.make_async_copy(o.at[pl.ds(0, ROW - 1)], m.at[pl.ds(0, ROW - 1)], rsemo.at[block]).wait()

        @pl.when(block > 0)
        def _():
            pltpu.make_async_copy(o.at[pl.ds(0, ROW)], m.at[pl.ds(0, ROW)], rsemo.at[block]).wait()

        piece = m[pl.ds(pl.multiple_of(came, ROW), ROW)].astype(F32).reshape(ROW * per, receivers)
        lines = pl.ds(pl.multiple_of(came * per, ROW * per), ROW * per)
        for q in range(receivers // LANES):
            m32[q, lines, :] = piece[:, q * LANES : (q + 1) * LANES]
        return carry

    lax.fori_loop(0, rows, collect, 0)
    scale2 = np.float32(1.0 / np.sqrt(size))
    stores = []
    for s in range(sources):
        parts = [
            jnp.concatenate([m32[q, pl.ds(c * sources + s, size, stride=per), :] for c in range(2)], axis=0)
            for q in range(receivers // LANES)
        ]
        lines = jnp.concatenate(parts, axis=1).astype(BF16)
        timed = lax.dot_general(lines, tab[...], (((0,), (0,)), ((), ())), preferred_element_type=F32)
        outv[s] = (timed * scale2).astype(BF16)
        store = pltpu.make_async_copy(outv.at[s], out_hbm.at[s], out_sem.at[s])
        store.start()
        stores.append(store)
    pltpu.make_async_copy(s23.at[pl.ds(0, size - 1)], r23.at[pl.ds(0, size - 1)], ssem23).wait()
    pltpu.make_async_copy(s1.at[pl.ds(0, size - 1)], r1.at[pl.ds(0, size - 1)], ssem1).wait()
    pltpu.make_async_copy(o.at[pl.ds(0, size - 1)], m.at[pl.ds(0, size - 1)], ssemo).wait()
    for store in stores:
        store.wait()


def on_device(size, p1, p2, p3, ws, we):
    sources, receivers, samples = p1.shape
    rows, per = size // ROW, 2 * sources
    vmem = pltpu.VMEM
    dma = pltpu.SemaphoreType.DMA
    return pl.pallas_call(
        functools.partial(kernel, size),
        out_shape=jax.ShapeDtypeStruct(p1.shape, BF16),
        in_specs=[pl.BlockSpec(memory_space=pl.ANY)] * 6,
        out_specs=pl.BlockSpec(memory_space=pl.ANY),
        scratch_shapes=[
            vmem((3,) + p1.shape, BF16),
            vmem(ws.shape, jnp.int32),
            vmem(we.shape, jnp.int32),
            vmem((2 * size, samples), BF16),
            vmem((receivers // LANES, 2 * per * size, LANES), F32),
            vmem((receivers // LANES, per * size, LANES), F32),
            vmem((size, 2 * per, receivers), BF16),
            vmem((size, per, receivers), BF16),
            vmem((size, 2 * per, receivers), BF16),
            vmem((size, per, receivers), BF16),
            vmem((size * per, receivers), BF16),
            vmem((size * per, receivers), BF16),
            vmem((size * per, receivers), BF16),
            vmem((receivers, 2 * receivers), BF16),
            vmem((size, per, receivers), BF16),
            vmem((size, per, receivers), BF16),
            vmem((receivers // LANES, size * per, LANES), F32),
            vmem(p1.shape, BF16),
            dma((6,)), dma((sources,)), dma, dma, dma, dma, dma((rows,)), dma((rows,)),
        ],
        compiler_params=pltpu.CompilerParams(
            collective_id=0, has_side_effects=True, vmem_limit_bytes=60 * 2**20
        ),
    )(p1, p2, p3, ws, we, jnp.asarray(make_table(size, samples)))


def solution(mesh):
    size = mesh.shape["freq"]
    spec = P(("groups", "freq"), None, None)
    wspec = P(None, ("groups", "freq"), None)
    return jax.shard_map(
        functools.partial(on_device, size),
        mesh=mesh,
        in_specs=(spec, spec, spec, wspec, wspec),
        out_specs=spec,
        check_vma=False,
    )
```

```python
import functools

import jax
import jax.numpy as jnp
import numpy as np
from jax import lax
from jax.experimental import pallas as pl
from jax.experimental.pallas import tpu as pltpu
from jax.sharding import PartitionSpec as P

MESH = pl.DeviceIdType.MESH
LANES = 128
ROW = 8
F32 = jnp.float32
BF16 = jnp.bfloat16


def make_table(count, samples):
    waves = np.arange(1, count + 1, dtype=np.int64)[:, None]
    times = np.arange(samples, dtype=np.int64)[None, :]
    angle = np.float32(2.0 * np.pi / samples) * (waves * times % samples).astype(np.float32)
    both = np.concatenate([np.cos(angle), -np.sin(angle)], axis=0)
    return both.astype(BF16)


def shift_of(block):
    return ((block + 1) // 2) * (2 * (block % 2) - 1)


def kernel(
    size, p1, p2, p3, ws, we, tab_hbm, m32, tab,
    inp, wsv, wev, a32, b32, s23, s1, r23, r1, xm, ym, zm, w, o, m,
    in_sem, ssem23, ssem1, ssemo, rsem23, rsem1, rsemo,
):
    me = lax.axis_index("freq")
    group = lax.axis_index("groups")
    rows = size // ROW
    z, xc = me // ROW, me % ROW
    samples = tab.shape[1]
    sources, receivers = inp.shape[1], inp.shape[2]
    per = 2 * sources

    barrier = pltpu.get_barrier_semaphore()

    def greet(k, carry):
        pl.semaphore_signal(barrier, inc=1, device_id=(group, (me + k) % size), device_id_type=MESH)
        return carry

    loads = [
        pltpu.make_async_copy(ws, wsv, in_sem.at[0]),
        pltpu.make_async_copy(we, wev, in_sem.at[1]),
        pltpu.make_async_copy(tab_hbm, tab, in_sem.at[2]),
        pltpu.make_async_copy(p2, inp.at[1], in_sem.at[4]),
        pltpu.make_async_copy(p3, inp.at[2], in_sem.at[5]),
        pltpu.make_async_copy(p1, inp.at[0], in_sem.at[3]),
    ]
    for load in loads:
        load.start()
    lax.fori_loop(1, size, greet, 0)
    for load in loads[:3]:
        load.wait()

    def spectra(j, into, base, stride):
        ends = jnp.concatenate([wsv[j], wev[j]], axis=0).astype(F32)
        columns = ends.T
        times = lax.broadcasted_iota(jnp.int32, (receivers, samples), 1).astype(F32)
        for s in range(sources):
            first = columns[:, s : s + 1]
            last = columns[:, sources + s : sources + s + 1]
            inside = (times >= first) & (times < last)
            traces = jnp.where(inside, inp[j, s].astype(F32), 0.0).astype(BF16)
            spec = lax.dot_general(tab[...], traces, (((1,), (1,)), ((), ())), preferred_element_type=F32)
            spec = spec * np.float32(1.0 / np.sqrt(samples))
            for c in range(2):
                for q in range(receivers // LANES):
                    into[q, pl.ds(base + c * sources + s, size, stride=stride), :] = spec[
                        c * size : (c + 1) * size, q * LANES : (q + 1) * LANES
                    ]

    def each_partner(body):
        def step(i, carry):
            block, turn = i // ROW, i % ROW
            dst = ((z + shift_of(block) + rows) % rows) * ROW + (xc + turn) % ROW
            body(block, dst)
            return carry

        lax.fori_loop(1, size, step, 0)

    loads[3].wait()
    spectra(1, a32, 0, 2 * per)
    loads[4].wait()
    spectra(2, a32, per, 2 * per)

    def round23(i, carry):
        at = pl.multiple_of(i * ROW, ROW)
        lines = pl.ds(pl.multiple_of(i * ROW * 2 * per, ROW * 2 * per), ROW * 2 * per)
        for q in range(receivers // LANES):
            piece = a32[q, lines, :].reshape(ROW, 2 * per, LANES)
            s23[pl.ds(at, ROW), :, q * LANES : (q + 1) * LANES] = piece.astype(BF16)
        return carry

    lax.fori_loop(0, rows, round23, 0)
    pl.semaphore_wait(barrier, size - 1)

    def send23(block, dst):
        pltpu.make_async_remote_copy(
            s23.at[dst], r23.at[me], ssem23, rsem23, device_id=(group, dst), device_id_type=MESH
        ).start()

    each_partner(send23)
    r23[me] = s23[me]

    loads[5].wait()
    spectra(0, b32, 0, per)

    def round1(i, carry):
        at = pl.multiple_of(i * ROW, ROW)
        lines = pl.ds(pl.multiple_of(i * ROW * per, ROW * per), ROW * per)
        for q in range(receivers // LANES):
            piece = b32[q, lines, :].reshape(ROW, per, LANES)
            s1[pl.ds(at, ROW), :, q * LANES : (q + 1) * LANES] = piece.astype(BF16)
        return carry

    lax.fori_loop(0, rows, round1, 0)

    def send1(block, dst):
        pltpu.make_async_remote_copy(
            s1.at[dst], r1.at[me], ssem1, rsem1.at[block], device_id=(group, dst), device_id_type=MESH
        ).start()

    each_partner(send1)
    r1[me] = s1[me]

    pltpu.make_async_copy(s23.at[pl.ds(0, size - 1)], r23.at[pl.ds(0, size - 1)], rsem23).wait()
    half = lax.broadcasted_iota(jnp.int32, (ROW, per, receivers), 1)
    sign = jnp.where(half < sources, 1.0, -1.0).astype(F32)

    def arrange(i, carry):
        at = pl.multiple_of(i * ROW, ROW)
        to = pl.ds(pl.multiple_of(i * ROW * per, ROW * per), ROW * per)
        piece = r23[pl.ds(at, ROW)].astype(F32)
        second, third = piece[:, :per], piece[:, per:]
        turned = jnp.concatenate([third[:, sources:], third[:, :sources]], axis=1) * sign
        xm[to, :] = second.reshape(ROW * per, receivers).astype(BF16)
        ym[to, :] = third.reshape(ROW * per, receivers).astype(BF16)
        zm[to, :] = turned.reshape(ROW * per, receivers).astype(BF16)
        return carry

    lax.fori_loop(0, rows, arrange, 0)
    scale = np.float32(1.0 / np.sqrt(size * sources))

    def weigh(i, carry):
        at = pl.ds(pl.multiple_of(i * LANES, LANES), LANES)
        left = xm[:, at]
        dims = (((0,), (0,)), ((), ()))
        w[at, :receivers] = (lax.dot_general(left, ym[...], dims, preferred_element_type=F32) * scale).astype(BF16)
        w[at, receivers:] = (lax.dot_general(left, zm[...], dims, preferred_element_type=F32) * scale).astype(BF16)
        return carry

    lax.fori_loop(0, receivers // LANES, weigh, 0)
    scale1 = np.float32(1.0 / np.sqrt(receivers))

    def multiply(block, carry):
        came = ((z - shift_of(block) + rows) % rows) * ROW

        @pl.when(block == 0)
        def _():
            pltpu.make_async_copy(s1.at[pl.ds(0, ROW - 1)], r1.at[pl.ds(0, ROW - 1)], rsem1.at[block]).wait()

        @pl.when(block > 0)
        def _():
            pltpu.make_async_copy(s1.at[pl.ds(0, ROW)], r1.at[pl.ds(0, ROW)], rsem1.at[block]).wait()

        at = pl.ds(pl.multiple_of(came, ROW), ROW)
        piece = r1[at].astype(F32).reshape(ROW * per, receivers).astype(BF16)
        both = jnp.dot(piece, w[...], preferred_element_type=F32)
        a = both[:, :receivers].reshape(ROW, per, receivers)
        b = both[:, receivers:].reshape(ROW, per, receivers)
        turned = jnp.concatenate([b[:, sources:], b[:, :sources]], axis=1) * sign
        o[at] = ((a - turned) * scale1).astype(BF16)

        def back(turn, c):
            dst = came + (xc + turn) % ROW

            @pl.when(dst != me)
            def _():
                pltpu.make_async_remote_copy(
                    o.at[dst], m.at[me], ssemo, rsemo.at[block], device_id=(group, dst), device_id_type=MESH
                ).start()

            return c

        lax.fori_loop(0, ROW, back, 0)
        return carry

    lax.fori_loop(0, rows, multiply, 0)
    m[me] = o[me]

    def collect(block, carry):
        came = ((z + shift_of(block) + rows) % rows) * ROW

        @pl.when(block == 0)
        def _():
            pltpu.make_async_copy(o.at[pl.ds(0, ROW - 1)], m.at[pl.ds(0, ROW - 1)], rsemo.at[block]).wait()

        @pl.when(block > 0)
        def _():
            pltpu.make_async_copy(o.at[pl.ds(0, ROW)], m.at[pl.ds(0, ROW)], rsemo.at[block]).wait()

        piece = m[pl.ds(pl.multiple_of(came, ROW), ROW)].astype(F32).reshape(ROW * per, receivers)
        lines = pl.ds(pl.multiple_of(came * per, ROW * per), ROW * per)
        for q in range(receivers // LANES):
            m32[q, lines, :] = piece[:, q * LANES : (q + 1) * LANES]
        return carry

    lax.fori_loop(0, rows, collect, 0)
    pltpu.make_async_copy(s23.at[pl.ds(0, size - 1)], r23.at[pl.ds(0, size - 1)], ssem23).wait()
    pltpu.make_async_copy(s1.at[pl.ds(0, size - 1)], r1.at[pl.ds(0, size - 1)], ssem1).wait()
    pltpu.make_async_copy(o.at[pl.ds(0, size - 1)], m.at[pl.ds(0, size - 1)], ssemo).wait()


def finish(size, m32, tab, out_hbm, outv, out_sem):
    sources, receivers = outv.shape[0], outv.shape[1]
    per = 2 * sources
    scale2 = np.float32(1.0 / np.sqrt(size))
    stores = []
    for s in range(sources):
        parts = [
            jnp.concatenate([m32[q, pl.ds(c * sources + s, size, stride=per), :] for c in range(2)], axis=0)
            for q in range(receivers // LANES)
        ]
        lines = jnp.concatenate(parts, axis=1).astype(BF16)
        timed = lax.dot_general(lines, tab[...], (((0,), (0,)), ((), ())), preferred_element_type=F32)
        outv[s] = (timed * scale2).astype(BF16)
        store = pltpu.make_async_copy(outv.at[s], out_hbm.at[s], out_sem.at[s])
        store.start()
        stores.append(store)
    for store in stores:
        store.wait()


def on_device(size, p1, p2, p3, ws, we):
    sources, receivers, samples = p1.shape
    rows, per = size // ROW, 2 * sources
    vmem = pltpu.VMEM
    dma = pltpu.SemaphoreType.DMA
    table = jnp.asarray(make_table(size, samples))
    lines, kept = pl.pallas_call(
        functools.partial(kernel, size),
        out_shape=(
            jax.ShapeDtypeStruct((receivers // LANES, size * per, LANES), F32),
            jax.ShapeDtypeStruct(table.shape, BF16),
        ),
        in_specs=[pl.BlockSpec(memory_space=pltpu.HBM)] * 6,
        out_specs=[pl.BlockSpec(memory_space=pltpu.VMEM)] * 2,
        scratch_shapes=[
            vmem((3,) + p1.shape, BF16),
            vmem(ws.shape, jnp.int32),
            vmem(we.shape, jnp.int32),
            vmem((receivers // LANES, 2 * per * size, LANES), F32),
            vmem((receivers // LANES, per * size, LANES), F32),
            vmem((size, 2 * per, receivers), BF16),
            vmem((size, per, receivers), BF16),
            vmem((size, 2 * per, receivers), BF16),
            vmem((size, per, receivers), BF16),
            vmem((size * per, receivers), BF16),
            vmem((size * per, receivers), BF16),
            vmem((size * per, receivers), BF16),
            vmem((receivers, 2 * receivers), BF16),
            vmem((size, per, receivers), BF16),
            vmem((size, per, receivers), BF16),
            dma((6,)), dma, dma, dma, dma, dma((rows,)), dma((rows,)),
        ],
        compiler_params=pltpu.CompilerParams(
            collective_id=0, has_side_effects=True, vmem_limit_bytes=50 * 2**20
        ),
    )(*(pltpu.with_memory_space_constraint(a, pltpu.HBM) for a in (p1, p2, p3, ws, we, table)))
    return pl.pallas_call(
        functools.partial(finish, size),
        out_shape=jax.ShapeDtypeStruct(p1.shape, BF16),
        in_specs=[pl.BlockSpec(memory_space=pltpu.VMEM)] * 2,
        out_specs=pl.BlockSpec(memory_space=pltpu.HBM),
        scratch_shapes=[vmem(p1.shape, BF16), dma((sources,))],
        compiler_params=pltpu.CompilerParams(vmem_limit_bytes=16 * 2**20),
    )(lines, kept)


def solution(mesh):
    size = mesh.shape["freq"]
    spec = P(("groups", "freq"), None, None)
    wspec = P(None, ("groups", "freq"), None)
    return jax.shard_map(
        functools.partial(on_device, size),
        mesh=mesh,
        in_specs=(spec, spec, spec, wspec, wspec),
        out_specs=spec,
        check_vma=False,
    )
```

```python
import functools

import jax
import jax.numpy as jnp
import numpy as np
from jax import lax
from jax.experimental import pallas as pl
from jax.experimental.pallas import tpu as pltpu
from jax.sharding import PartitionSpec as P

MESH = pl.DeviceIdType.MESH
LANES = 128
ROW = 8
F32 = jnp.float32
BF16 = jnp.bfloat16


def make_table(count, samples):
    waves = np.arange(1, count + 1, dtype=np.int64)[:, None]
    times = np.arange(samples, dtype=np.int64)[None, :]
    angle = np.float32(2.0 * np.pi / samples) * (waves * times % samples).astype(np.float32)
    both = np.concatenate([np.cos(angle), -np.sin(angle)], axis=0)
    return both.astype(BF16)


def shift_of(block):
    return ((block + 1) // 2) * (2 * (block % 2) - 1)


def kernel(
    size, p1, p2, p3, ws, we, tab_hbm, m32, tab,
    inp, wsv, wev, a32, b32, s23, s1, r23, r1, xm, ym, zm, w, o, m,
    in_sem, ssem23, ssem1, ssemo, rsem23, rsem1, rsemo, up, last_in,
):
    me = lax.axis_index("freq")
    group = lax.axis_index("groups")
    rows = size // ROW
    z, xc = me // ROW, me % ROW
    samples = tab.shape[1]
    sources, receivers = inp.shape[1], inp.shape[2]
    per = 2 * sources

    barrier = pltpu.get_barrier_semaphore()

    def greet(turn, carry):
        mate = z * ROW + (xc + turn) % ROW

        @pl.when(mate != 0)
        def _():
            pl.semaphore_signal(barrier, inc=1, device_id=(group, mate), device_id_type=MESH)

        return carry

    def report(below, carry):
        target = below * ROW + xc

        @pl.when(target != 0)
        def _():
            pl.semaphore_signal(up.at[z], inc=1, device_id=(group, target), device_id_type=MESH)

        return carry

    def announce(turn, carry):
        mate = z * ROW + (xc + turn) % ROW
        pl.semaphore_signal(last_in, inc=1, device_id=(group, mate), device_id_type=MESH)
        return carry

    def announce_row(row, carry):
        pl.semaphore_signal(last_in, inc=1, device_id=(group, row * ROW), device_id_type=MESH)
        return carry

    loads = [
        pltpu.make_async_copy(ws, wsv, in_sem.at[0]),
        pltpu.make_async_copy(we, wev, in_sem.at[1]),
        pltpu.make_async_copy(tab_hbm, tab, in_sem.at[2]),
        pltpu.make_async_copy(p2, inp.at[1], in_sem.at[4]),
        pltpu.make_async_copy(p3, inp.at[2], in_sem.at[5]),
        pltpu.make_async_copy(p1, inp.at[0], in_sem.at[3]),
    ]
    for load in loads:
        load.start()

    @pl.when(me != 0)
    def _():
        lax.fori_loop(1, ROW, greet, 0)
        pl.semaphore_wait(barrier, ROW - 2 + 2 * jnp.minimum(z, 1))

        @pl.when(z < rows - 1)
        def _():
            pl.semaphore_signal(barrier, inc=1, device_id=(group, me + ROW), device_id_type=MESH)

        @pl.when(me == 1)
        def _():
            pl.semaphore_signal(barrier, inc=1, device_id=(group, ROW), device_id_type=MESH)

        @pl.when(me == size - ROW)
        def _():
            pl.semaphore_signal(barrier, inc=1, device_id=(group, 0), device_id_type=MESH)

        lax.fori_loop(0, z, report, 0)

    for load in loads[:3]:
        load.wait()

    def spectra(j, into, base, stride):
        ends = jnp.concatenate([wsv[j], wev[j]], axis=0).astype(F32)
        columns = ends.T
        times = lax.broadcasted_iota(jnp.int32, (receivers, samples), 1).astype(F32)
        for s in range(sources):
            first = columns[:, s : s + 1]
            last = columns[:, sources + s : sources + s + 1]
            inside = (times >= first) & (times < last)
            traces = jnp.where(inside, inp[j, s].astype(F32), 0.0).astype(BF16)
            spec = lax.dot_general(tab[...], traces, (((1,), (1,)), ((), ())), preferred_element_type=F32)
            spec = spec * np.float32(1.0 / np.sqrt(samples))
            for c in range(2):
                for q in range(receivers // LANES):
                    into[q, pl.ds(base + c * sources + s, size, stride=stride), :] = spec[
                        c * size : (c + 1) * size, q * LANES : (q + 1) * LANES
                    ]

    def each_partner(body):
        def step(i, carry):
            block, turn = i // ROW, i % ROW
            dst = ((z + shift_of(block) + rows) % rows) * ROW + (xc + turn) % ROW
            body(block, dst)
            return carry

        lax.fori_loop(1, size, step, 0)

    loads[3].wait()
    spectra(1, a32, 0, 2 * per)
    loads[4].wait()
    spectra(2, a32, per, 2 * per)

    def partner_row(block):
        return (z + shift_of(block) + rows) % rows

    def round23(row):
        lines = pl.ds(pl.multiple_of(row * ROW * 2 * per, ROW * 2 * per), ROW * 2 * per)
        for q in range(receivers // LANES):
            piece = a32[q, lines, :].reshape(ROW, 2 * per, LANES)
            s23[pl.ds(pl.multiple_of(row * ROW, ROW), ROW), :, q * LANES : (q + 1) * LANES] = piece.astype(BF16)

    def send23_to(dst):
        pltpu.make_async_remote_copy(
            s23.at[dst], r23.at[me], ssem23, rsem23, device_id=(group, dst), device_id_type=MESH
        ).start()

    def send23(row):
        def step(turn, carry):
            dst = row * ROW + (xc + turn) % ROW

            @pl.when((dst != me) & (dst != 0))
            def _():
                send23_to(dst)

            return carry

        lax.fori_loop(0, ROW, step, 0)

    round23(z)

    @pl.when(me == 0)
    def _():
        pl.semaphore_wait(barrier, 1)
        lax.fori_loop(1, rows, announce_row, 0)
        lax.fori_loop(1, ROW, announce, 0)

    def early(block, carry):
        @pl.when(block < rows - 1)
        def _():
            round23(partner_row((block + 1) % rows))

        @pl.when(partner_row(block) <= z)
        def _():
            send23(partner_row(block))

        return carry

    lax.fori_loop(0, rows, early, 0)
    r23[me] = s23[me]

    loads[5].wait()
    spectra(0, b32, 0, per)

    def round1(i, carry):
        at = pl.multiple_of(i * ROW, ROW)
        lines = pl.ds(pl.multiple_of(i * ROW * per, ROW * per), ROW * per)
        for q in range(receivers // LANES):
            piece = b32[q, lines, :].reshape(ROW, per, LANES)
            s1[pl.ds(at, ROW), :, q * LANES : (q + 1) * LANES] = piece.astype(BF16)
        return carry

    lax.fori_loop(0, rows, round1, 0)

    def late(row, carry):
        @pl.when(me != 0)
        def _():
            pl.semaphore_wait(up.at[row], 1)

        send23(row)
        return carry

    lax.fori_loop(z + 1, rows, late, 0)

    @pl.when(me != 0)
    def _():
        pl.semaphore_wait(last_in, 1)

        @pl.when(xc == 0)
        def _():
            lax.fori_loop(1, ROW, announce, 0)

        send23_to(0)

    def send1(block, dst):
        pltpu.make_async_remote_copy(
            s1.at[dst], r1.at[me], ssem1, rsem1.at[block], device_id=(group, dst), device_id_type=MESH
        ).start()

    each_partner(send1)
    r1[me] = s1[me]

    pltpu.make_async_copy(s23.at[pl.ds(0, size - 1)], r23.at[pl.ds(0, size - 1)], rsem23).wait()
    half = lax.broadcasted_iota(jnp.int32, (ROW, per, receivers), 1)
    sign = jnp.where(half < sources, 1.0, -1.0).astype(F32)

    def arrange(i, carry):
        at = pl.multiple_of(i * ROW, ROW)
        to = pl.ds(pl.multiple_of(i * ROW * per, ROW * per), ROW * per)
        piece = r23[pl.ds(at, ROW)].astype(F32)
        second, third = piece[:, :per], piece[:, per:]
        turned = jnp.concatenate([third[:, sources:], third[:, :sources]], axis=1) * sign
        xm[to, :] = second.reshape(ROW * per, receivers).astype(BF16)
        ym[to, :] = third.reshape(ROW * per, receivers).astype(BF16)
        zm[to, :] = turned.reshape(ROW * per, receivers).astype(BF16)
        return carry

    lax.fori_loop(0, rows, arrange, 0)
    scale = np.float32(1.0 / np.sqrt(size * sources))

    def weigh(i, carry):
        at = pl.ds(pl.multiple_of(i * LANES, LANES), LANES)
        left = xm[:, at]
        dims = (((0,), (0,)), ((), ()))
        w[at, :receivers] = (lax.dot_general(left, ym[...], dims, preferred_element_type=F32) * scale).astype(BF16)
        w[at, receivers:] = (lax.dot_general(left, zm[...], dims, preferred_element_type=F32) * scale).astype(BF16)
        return carry

    lax.fori_loop(0, receivers // LANES, weigh, 0)
    scale1 = np.float32(1.0 / np.sqrt(receivers))

    def multiply(block, carry):
        came = ((z - shift_of(block) + rows) % rows) * ROW

        @pl.when(block == 0)
        def _():
            pltpu.make_async_copy(s1.at[pl.ds(0, ROW - 1)], r1.at[pl.ds(0, ROW - 1)], rsem1.at[block]).wait()

        @pl.when(block > 0)
        def _():
            pltpu.make_async_copy(s1.at[pl.ds(0, ROW)], r1.at[pl.ds(0, ROW)], rsem1.at[block]).wait()

        at = pl.ds(pl.multiple_of(came, ROW), ROW)
        piece = r1[at].astype(F32).reshape(ROW * per, receivers).astype(BF16)
        both = jnp.dot(piece, w[...], preferred_element_type=F32)
        a = both[:, :receivers].reshape(ROW, per, receivers)
        b = both[:, receivers:].reshape(ROW, per, receivers)
        turned = jnp.concatenate([b[:, sources:], b[:, :sources]], axis=1) * sign
        o[at] = ((a - turned) * scale1).astype(BF16)

        def back(turn, c):
            dst = came + (xc + turn) % ROW

            @pl.when(dst != me)
            def _():
                pltpu.make_async_remote_copy(
                    o.at[dst], m.at[me], ssemo, rsemo.at[block], device_id=(group, dst), device_id_type=MESH
                ).start()

            return c

        lax.fori_loop(0, ROW, back, 0)
        return carry

    lax.fori_loop(0, rows, multiply, 0)
    m[me] = o[me]

    def collect(block, carry):
        came = ((z + shift_of(block) + rows) % rows) * ROW

        @pl.when(block == 0)
        def _():
            pltpu.make_async_copy(o.at[pl.ds(0, ROW - 1)], m.at[pl.ds(0, ROW - 1)], rsemo.at[block]).wait()

        @pl.when(block > 0)
        def _():
            pltpu.make_async_copy(o.at[pl.ds(0, ROW)], m.at[pl.ds(0, ROW)], rsemo.at[block]).wait()

        piece = m[pl.ds(pl.multiple_of(came, ROW), ROW)].astype(F32).reshape(ROW * per, receivers)
        lines = pl.ds(pl.multiple_of(came * per, ROW * per), ROW * per)
        for q in range(receivers // LANES):
            m32[q, lines, :] = piece[:, q * LANES : (q + 1) * LANES]
        return carry

    lax.fori_loop(0, rows, collect, 0)
    pltpu.make_async_copy(s23.at[pl.ds(0, size - 1)], r23.at[pl.ds(0, size - 1)], ssem23).wait()
    pltpu.make_async_copy(s1.at[pl.ds(0, size - 1)], r1.at[pl.ds(0, size - 1)], ssem1).wait()
    pltpu.make_async_copy(o.at[pl.ds(0, size - 1)], m.at[pl.ds(0, size - 1)], ssemo).wait()


def finish(size, m32, tab, out_hbm, outv, out_sem):
    sources, receivers = outv.shape[0], outv.shape[1]
    per = 2 * sources
    scale2 = np.float32(1.0 / np.sqrt(size))
    stores = []
    for s in range(sources):
        parts = [
            jnp.concatenate([m32[q, pl.ds(c * sources + s, size, stride=per), :] for c in range(2)], axis=0)
            for q in range(receivers // LANES)
        ]
        lines = jnp.concatenate(parts, axis=1).astype(BF16)
        timed = lax.dot_general(lines, tab[...], (((0,), (0,)), ((), ())), preferred_element_type=F32)
        outv[s] = (timed * scale2).astype(BF16)
        store = pltpu.make_async_copy(outv.at[s], out_hbm.at[s], out_sem.at[s])
        store.start()
        stores.append(store)
    for store in stores:
        store.wait()


def on_device(size, p1, p2, p3, ws, we):
    sources, receivers, samples = p1.shape
    rows, per = size // ROW, 2 * sources
    vmem = pltpu.VMEM
    dma = pltpu.SemaphoreType.DMA
    table = jnp.asarray(make_table(size, samples))
    lines, kept = pl.pallas_call(
        functools.partial(kernel, size),
        out_shape=(
            jax.ShapeDtypeStruct((receivers // LANES, size * per, LANES), F32),
            jax.ShapeDtypeStruct(table.shape, BF16),
        ),
        in_specs=[pl.BlockSpec(memory_space=pltpu.HBM)] * 6,
        out_specs=[pl.BlockSpec(memory_space=pltpu.VMEM)] * 2,
        scratch_shapes=[
            vmem((3,) + p1.shape, BF16),
            vmem(ws.shape, jnp.int32),
            vmem(we.shape, jnp.int32),
            vmem((receivers // LANES, 2 * per * size, LANES), F32),
            vmem((receivers // LANES, per * size, LANES), F32),
            vmem((size, 2 * per, receivers), BF16),
            vmem((size, per, receivers), BF16),
            vmem((size, 2 * per, receivers), BF16),
            vmem((size, per, receivers), BF16),
            vmem((size * per, receivers), BF16),
            vmem((size * per, receivers), BF16),
            vmem((size * per, receivers), BF16),
            vmem((receivers, 2 * receivers), BF16),
            vmem((size, per, receivers), BF16),
            vmem((size, per, receivers), BF16),
            dma((6,)), dma, dma, dma, dma, dma((rows,)), dma((rows,)),
            pltpu.SemaphoreType.REGULAR((rows,)), pltpu.SemaphoreType.REGULAR,
        ],
        compiler_params=pltpu.CompilerParams(
            collective_id=0, has_side_effects=True, vmem_limit_bytes=50 * 2**20
        ),
    )(*(pltpu.with_memory_space_constraint(a, pltpu.HBM) for a in (p1, p2, p3, ws, we, table)))
    return pl.pallas_call(
        functools.partial(finish, size),
        out_shape=jax.ShapeDtypeStruct(p1.shape, BF16),
        in_specs=[pl.BlockSpec(memory_space=pltpu.VMEM)] * 2,
        out_specs=pl.BlockSpec(memory_space=pltpu.HBM),
        scratch_shapes=[vmem(p1.shape, BF16), dma((sources,))],
        compiler_params=pltpu.CompilerParams(vmem_limit_bytes=16 * 2**20),
    )(lines, kept)


def solution(mesh):
    size = mesh.shape["freq"]
    spec = P(("groups", "freq"), None, None)
    wspec = P(None, ("groups", "freq"), None)
    return jax.shard_map(
        functools.partial(on_device, size),
        mesh=mesh,
        in_specs=(spec, spec, spec, wspec, wspec),
        out_specs=spec,
        check_vma=False,
    )
```

```python
import functools

import jax
import jax.numpy as jnp
import numpy as np
from jax import lax
from jax.experimental import pallas as pl
from jax.experimental.pallas import tpu as pltpu
from jax.sharding import PartitionSpec as P

MESH = pl.DeviceIdType.MESH
LANES = 128
ROW = 8
F32 = jnp.float32
BF16 = jnp.bfloat16


def make_table(count, samples):
    waves = np.arange(1, count + 1, dtype=np.int64)[:, None]
    times = np.arange(samples, dtype=np.int64)[None, :]
    angle = np.float32(2.0 * np.pi / samples) * (waves * times % samples).astype(np.float32)
    both = np.concatenate([np.cos(angle), -np.sin(angle)], axis=0)
    return both.astype(BF16)


def shift_of(block):
    return ((block + 1) // 2) * (2 * (block % 2) - 1)


def kernel(
    size, p1, p2, p3, ws, we, tab_hbm, m32, tab,
    inp, wsv, wev, a32, b32, s23, s1, r23, r1, xm, ym, zm, w, o, m,
    in_sem, ssem23, ssem1, ssemo, rsem23, rsem1, rsemo, up, last_in,
):
    me = lax.axis_index("freq")
    group = lax.axis_index("groups")
    rows = size // ROW
    z, xc = me // ROW, me % ROW
    samples = tab.shape[1]
    sources, receivers = inp.shape[1], inp.shape[2]
    per = 2 * sources

    barrier = pltpu.get_barrier_semaphore()

    def greet(turn, carry):
        mate = z * ROW + (xc + turn) % ROW

        @pl.when(mate != 0)
        def _():
            pl.semaphore_signal(barrier, inc=1, device_id=(group, mate), device_id_type=MESH)

        return carry

    def report(below, carry):
        target = below * ROW + xc

        @pl.when(target != 0)
        def _():
            pl.semaphore_signal(up.at[z], inc=1, device_id=(group, target), device_id_type=MESH)

        return carry

    def announce(turn, carry):
        mate = z * ROW + (xc + turn) % ROW
        pl.semaphore_signal(last_in, inc=1, device_id=(group, mate), device_id_type=MESH)
        return carry

    def announce_row(row, carry):
        pl.semaphore_signal(last_in, inc=1, device_id=(group, row * ROW), device_id_type=MESH)
        return carry

    loads = [
        pltpu.make_async_copy(ws, wsv, in_sem.at[0]),
        pltpu.make_async_copy(we, wev, in_sem.at[1]),
        pltpu.make_async_copy(tab_hbm, tab, in_sem.at[2]),
        pltpu.make_async_copy(p2, inp.at[1], in_sem.at[4]),
        pltpu.make_async_copy(p3, inp.at[2], in_sem.at[5]),
        pltpu.make_async_copy(p1, inp.at[0], in_sem.at[3]),
    ]
    for load in loads:
        load.start()

    @pl.when(me != 0)
    def _():
        lax.fori_loop(1, ROW, greet, 0)
        pl.semaphore_wait(barrier, ROW - 2 + 2 * jnp.minimum(z, 1))

        @pl.when(z < rows - 1)
        def _():
            pl.semaphore_signal(barrier, inc=1, device_id=(group, me + ROW), device_id_type=MESH)

        @pl.when(me == 1)
        def _():
            pl.semaphore_signal(barrier, inc=1, device_id=(group, ROW), device_id_type=MESH)

        @pl.when(me == size - ROW)
        def _():
            pl.semaphore_signal(barrier, inc=1, device_id=(group, 0), device_id_type=MESH)

        lax.fori_loop(0, z, report, 0)

    for load in loads[:3]:
        load.wait()

    def spectra(j, into, base, stride):
        ends = jnp.concatenate([wsv[j], wev[j]], axis=0).astype(F32)
        columns = ends.T
        times = lax.broadcasted_iota(jnp.int32, (receivers, samples), 1).astype(F32)
        for s in range(sources):
            first = columns[:, s : s + 1]
            last = columns[:, sources + s : sources + s + 1]
            inside = (times >= first) & (times < last)
            traces = jnp.where(inside, inp[j, s].astype(F32), 0.0).astype(BF16)
            spec = lax.dot_general(tab[...], traces, (((1,), (1,)), ((), ())), preferred_element_type=F32)
            spec = spec * np.float32(1.0 / np.sqrt(samples))
            for c in range(2):
                for q in range(receivers // LANES):
                    into[q, pl.ds(base + c * sources + s, size, stride=stride), :] = spec[
                        c * size : (c + 1) * size, q * LANES : (q + 1) * LANES
                    ]

    def each_partner(body):
        def step(i, carry):
            block, turn = i // ROW, i % ROW
            dst = ((z + shift_of(block) + rows) % rows) * ROW + (xc + turn) % ROW
            body(block, dst)
            return carry

        lax.fori_loop(1, size, step, 0)

    loads[3].wait()
    spectra(1, a32, 0, 2 * per)
    loads[4].wait()
    spectra(2, a32, per, 2 * per)

    def partner_row(block):
        return (z + shift_of(block) + rows) % rows

    def round23(row):
        lines = pl.ds(pl.multiple_of(row * ROW * 2 * per, ROW * 2 * per), ROW * 2 * per)
        for q in range(receivers // LANES):
            piece = a32[q, lines, :].reshape(ROW, 2 * per, LANES)
            s23[pl.ds(pl.multiple_of(row * ROW, ROW), ROW), :, q * LANES : (q + 1) * LANES] = piece.astype(BF16)

    def send23_to(dst):
        pltpu.make_async_remote_copy(
            s23.at[dst], r23.at[me], ssem23, rsem23, device_id=(group, dst), device_id_type=MESH
        ).start()

    def send23(row):
        def step(turn, carry):
            dst = row * ROW + (xc + turn) % ROW

            @pl.when((dst != me) & (dst != 0))
            def _():
                send23_to(dst)

            return carry

        lax.fori_loop(0, ROW, step, 0)

    round23(z)

    @pl.when(me == 0)
    def _():
        pl.semaphore_wait(barrier, 1)
        lax.fori_loop(1, rows, announce_row, 0)
        lax.fori_loop(1, ROW, announce, 0)

    def early(block, carry):
        @pl.when(block < rows - 1)
        def _():
            round23(partner_row((block + 1) % rows))

        @pl.when(partner_row(block) <= z)
        def _():
            send23(partner_row(block))

        return carry

    lax.fori_loop(0, rows, early, 0)
    r23[me] = s23[me]

    loads[5].wait()
    spectra(0, b32, 0, per)

    def round1(i, carry):
        at = pl.multiple_of(i * ROW, ROW)
        lines = pl.ds(pl.multiple_of(i * ROW * per, ROW * per), ROW * per)
        for q in range(receivers // LANES):
            piece = b32[q, lines, :].reshape(ROW, per, LANES)
            s1[pl.ds(at, ROW), :, q * LANES : (q + 1) * LANES] = piece.astype(BF16)
        return carry

    lax.fori_loop(0, rows, round1, 0)

    def late(row, carry):
        @pl.when(me != 0)
        def _():
            pl.semaphore_wait(up.at[row], 1)

        send23(row)
        return carry

    lax.fori_loop(z + 1, rows, late, 0)

    @pl.when(me != 0)
    def _():
        pl.semaphore_wait(last_in, 1)

        @pl.when(xc == 0)
        def _():
            lax.fori_loop(1, ROW, announce, 0)

        send23_to(0)

    def send1(block, dst):
        pltpu.make_async_remote_copy(
            s1.at[dst], r1.at[me], ssem1, rsem1.at[block], device_id=(group, dst), device_id_type=MESH
        ).start()

    each_partner(send1)
    r1[me] = s1[me]

    pltpu.make_async_copy(s23.at[pl.ds(0, size - 1)], r23.at[pl.ds(0, size - 1)], rsem23).wait()
    half = lax.broadcasted_iota(jnp.int32, (ROW, per, receivers), 1)
    sign = jnp.where(half < sources, 1.0, -1.0).astype(F32)

    def arrange(i, carry):
        at = pl.multiple_of(i * ROW, ROW)
        to = pl.ds(pl.multiple_of(i * ROW * per, ROW * per), ROW * per)
        piece = r23[pl.ds(at, ROW)].astype(F32)
        second, third = piece[:, :per], piece[:, per:]
        turned = jnp.concatenate([third[:, sources:], third[:, :sources]], axis=1) * sign
        xm[to, :] = second.reshape(ROW * per, receivers).astype(BF16)
        ym[to, :] = third.reshape(ROW * per, receivers).astype(BF16)
        zm[to, :] = turned.reshape(ROW * per, receivers).astype(BF16)
        return carry

    lax.fori_loop(0, rows, arrange, 0)
    scale = np.float32(1.0 / np.sqrt(size * sources))

    def weigh(i, carry):
        at = pl.ds(pl.multiple_of(i * LANES, LANES), LANES)
        left = xm[:, at]
        dims = (((0,), (0,)), ((), ()))
        w[at, :receivers] = (lax.dot_general(left, ym[...], dims, preferred_element_type=F32) * scale).astype(BF16)
        w[at, receivers:] = (lax.dot_general(left, zm[...], dims, preferred_element_type=F32) * scale).astype(BF16)
        return carry

    lax.fori_loop(0, receivers // LANES, weigh, 0)
    scale1 = np.float32(1.0 / np.sqrt(receivers))

    def multiply(i, carry):
        gap = (z - i + rows) % rows
        block = jnp.where(gap <= rows // 2, 2 * gap - 1, 2 * (rows - gap))
        block = jnp.where(gap == 0, 0, block)
        came = ((z - shift_of(block) + rows) % rows) * ROW

        @pl.when(block == 0)
        def _():
            pltpu.make_async_copy(s1.at[pl.ds(0, ROW - 1)], r1.at[pl.ds(0, ROW - 1)], rsem1.at[block]).wait()

        @pl.when(block > 0)
        def _():
            pltpu.make_async_copy(s1.at[pl.ds(0, ROW)], r1.at[pl.ds(0, ROW)], rsem1.at[block]).wait()

        at = pl.ds(pl.multiple_of(came, ROW), ROW)
        piece = r1[at].astype(F32).reshape(ROW * per, receivers).astype(BF16)
        both = jnp.dot(piece, w[...], preferred_element_type=F32)
        a = both[:, :receivers].reshape(ROW, per, receivers)
        b = both[:, receivers:].reshape(ROW, per, receivers)
        turned = jnp.concatenate([b[:, sources:], b[:, :sources]], axis=1) * sign
        o[at] = ((a - turned) * scale1).astype(BF16)

        def back(turn, c):
            dst = came + (xc + turn) % ROW

            @pl.when(dst != me)
            def _():
                pltpu.make_async_remote_copy(
                    o.at[dst], m.at[me], ssemo, rsemo.at[block], device_id=(group, dst), device_id_type=MESH
                ).start()

            return c

        lax.fori_loop(0, ROW, back, 0)
        return carry

    lax.fori_loop(0, rows, multiply, 0)
    m[me] = o[me]

    def collect(block, carry):
        came = ((z + shift_of(block) + rows) % rows) * ROW

        @pl.when(block == 0)
        def _():
            pltpu.make_async_copy(o.at[pl.ds(0, ROW - 1)], m.at[pl.ds(0, ROW - 1)], rsemo.at[block]).wait()

        @pl.when(block > 0)
        def _():
            pltpu.make_async_copy(o.at[pl.ds(0, ROW)], m.at[pl.ds(0, ROW)], rsemo.at[block]).wait()

        piece = m[pl.ds(pl.multiple_of(came, ROW), ROW)].astype(F32).reshape(ROW * per, receivers)
        lines = pl.ds(pl.multiple_of(came * per, ROW * per), ROW * per)
        for q in range(receivers // LANES):
            m32[q, lines, :] = piece[:, q * LANES : (q + 1) * LANES]
        return carry

    lax.fori_loop(0, rows, collect, 0)
    pltpu.make_async_copy(s23.at[pl.ds(0, size - 1)], r23.at[pl.ds(0, size - 1)], ssem23).wait()
    pltpu.make_async_copy(s1.at[pl.ds(0, size - 1)], r1.at[pl.ds(0, size - 1)], ssem1).wait()
    pltpu.make_async_copy(o.at[pl.ds(0, size - 1)], m.at[pl.ds(0, size - 1)], ssemo).wait()


def finish(size, m32, tab, out_hbm, outv, out_sem):
    sources, receivers = outv.shape[0], outv.shape[1]
    per = 2 * sources
    scale2 = np.float32(1.0 / np.sqrt(size))
    stores = []
    for s in range(sources):
        parts = [
            jnp.concatenate([m32[q, pl.ds(c * sources + s, size, stride=per), :] for c in range(2)], axis=0)
            for q in range(receivers // LANES)
        ]
        lines = jnp.concatenate(parts, axis=1).astype(BF16)
        timed = lax.dot_general(lines, tab[...], (((0,), (0,)), ((), ())), preferred_element_type=F32)
        outv[s] = (timed * scale2).astype(BF16)
        store = pltpu.make_async_copy(outv.at[s], out_hbm.at[s], out_sem.at[s])
        store.start()
        stores.append(store)
    for store in stores:
        store.wait()


def on_device(size, p1, p2, p3, ws, we):
    sources, receivers, samples = p1.shape
    rows, per = size // ROW, 2 * sources
    vmem = pltpu.VMEM
    dma = pltpu.SemaphoreType.DMA
    table = jnp.asarray(make_table(size, samples))
    lines, kept = pl.pallas_call(
        functools.partial(kernel, size),
        out_shape=(
            jax.ShapeDtypeStruct((receivers // LANES, size * per, LANES), F32),
            jax.ShapeDtypeStruct(table.shape, BF16),
        ),
        in_specs=[pl.BlockSpec(memory_space=pltpu.HBM)] * 6,
        out_specs=[pl.BlockSpec(memory_space=pltpu.VMEM)] * 2,
        scratch_shapes=[
            vmem((3,) + p1.shape, BF16),
            vmem(ws.shape, jnp.int32),
            vmem(we.shape, jnp.int32),
            vmem((receivers // LANES, 2 * per * size, LANES), F32),
            vmem((receivers // LANES, per * size, LANES), F32),
            vmem((size, 2 * per, receivers), BF16),
            vmem((size, per, receivers), BF16),
            vmem((size, 2 * per, receivers), BF16),
            vmem((size, per, receivers), BF16),
            vmem((size * per, receivers), BF16),
            vmem((size * per, receivers), BF16),
            vmem((size * per, receivers), BF16),
            vmem((receivers, 2 * receivers), BF16),
            vmem((size, per, receivers), BF16),
            vmem((size, per, receivers), BF16),
            dma((6,)), dma, dma, dma, dma, dma((rows,)), dma((rows,)),
            pltpu.SemaphoreType.REGULAR((rows,)), pltpu.SemaphoreType.REGULAR,
        ],
        compiler_params=pltpu.CompilerParams(
            collective_id=0, has_side_effects=True, vmem_limit_bytes=50 * 2**20
        ),
    )(*(pltpu.with_memory_space_constraint(a, pltpu.HBM) for a in (p1, p2, p3, ws, we, table)))
    return pl.pallas_call(
        functools.partial(finish, size),
        out_shape=jax.ShapeDtypeStruct(p1.shape, BF16),
        in_specs=[pl.BlockSpec(memory_space=pltpu.VMEM)] * 2,
        out_specs=pl.BlockSpec(memory_space=pltpu.HBM),
        scratch_shapes=[vmem(p1.shape, BF16), dma((sources,))],
        compiler_params=pltpu.CompilerParams(vmem_limit_bytes=16 * 2**20),
    )(lines, kept)


def solution(mesh):
    size = mesh.shape["freq"]
    spec = P(("groups", "freq"), None, None)
    wspec = P(None, ("groups", "freq"), None)
    return jax.shard_map(
        functools.partial(on_device, size),
        mesh=mesh,
        in_specs=(spec, spec, spec, wspec, wspec),
        out_specs=spec,
        check_vma=False,
    )
```
